32 devices in a mesh: seq: 8 (over y, x, core), fsdp: 4 (over z).
Axes of the slice: x: 2, y: 2, z: 4, core: 2. Of those that a mesh axis runs over, the one named last changes fastest.
Arguments:
- hidden_in: bfloat16 [4, 1536, 2048], P('fsdp', 'seq'), may hold values from -6 to 6
- weight_query: bfloat16 [2048, 2048], P(('seq', 'fsdp')), may hold values from -0.125 to 0.125
- weight_key: bfloat16 [2048, 2048], P(('seq', 'fsdp')), may hold values from -0.125 to 0.125
- weight_value: bfloat16 [2048, 2048], P(('seq', 'fsdp')), may hold values from -0.125 to 0.125
- weight_output: bfloat16 [2048, 2048], P(('seq', 'fsdp')), may hold values from -2 to 2
- weight_router: bfloat16 [2048, 32], P(('seq', 'fsdp')), may hold values from -0.0625 to 0.0625
- attention_gain: bfloat16 [2048], P(('seq', 'fsdp')), may hold values from 0.5 to 1.5
- mixture_gain: bfloat16 [2048], P(('seq', 'fsdp')), may hold values from 0.5 to 1.5
- queries_gain: bfloat16 [2048], P(('seq', 'fsdp')), may hold values from 0.5 to 1.5
- keys_gain: bfloat16 [2048], P(('seq', 'fsdp')), may hold values from 0.5 to 1.5
- weight_gate: bfloat16 [32, 2048, 1024], P('seq', 'fsdp'), may hold values from -0.125 to 0.125
- weight_up: bfloat16 [32, 2048, 1024], P('seq', 'fsdp'), may hold values from -0.125 to 0.125
- weight_down: bfloat16 [32, 1024, 2048], P('seq', 'fsdp'), may hold values from -0.75 to 0.75
- cotangent: bfloat16 [4, 1536, 2048], P('fsdp', 'seq'), may hold values from -6 to 6
- token_order: int32 [4, 1536], P('fsdp'), may hold values from 0 to 1535, each once within a row
- sequence_lengths: int32 [4, 2], P('fsdp'), may hold values from 1 to 1024, 1536 in all within a row
- expert_choice: int32 [4, 1536, 8], P('fsdp', 'seq'), may hold values from 0 to 31, all different within a row
Outputs:
- block_out: bfloat16 [4, 1536, 2048], P('fsdp', 'seq')
- grad_hidden: bfloat16 [4, 1536, 2048], P('fsdp', 'seq')
- grad_query: float32 [2048, 2048], P(('seq', 'fsdp'))
- grad_key: float32 [2048, 2048], P(('seq', 'fsdp'))
- grad_value: float32 [2048, 2048], P(('seq', 'fsdp'))
- grad_output: float32 [2048, 2048], P(('seq', 'fsdp'))
- grad_router: float32 [2048, 32], P(('seq', 'fsdp'))
- grad_attention_gain: float32 [2048], P(('seq', 'fsdp'))
- grad_mixture_gain: float32 [2048], P(('seq', 'fsdp'))
- grad_queries_gain: float32 [2048], P(('seq', 'fsdp'))
- grad_keys_gain: float32 [2048], P(('seq', 'fsdp'))
- grad_gate: float32 [32, 2048, 1024], P('seq', 'fsdp')
- grad_up: float32 [32, 2048, 1024], P('seq', 'fsdp')
- grad_down: float32 [32, 1024, 2048], P('seq', 'fsdp')
The draws below stay inside these ranges and needn't reach their ends.
Inputs may be any that keep to these rules, and one draw needn't show every extreme that they name: Each group's row of token_order is a permutation. `sequence_lengths`: each group's lengths sum to 1536; none is longer than 1024. `expert_choice`: a token names 8 different experts; every expert is named by some token.
All inputs are finite; a program needn't handle non-finite values.
Results may differ from the reference program's by a relative error of at most 0.017.
Values may be sent and summed in bfloat16 or wider, within the bound.
A program may use at most 384 MiB of HBM per device.

```python
import math
import jax
import jax.numpy as jnp
import numpy as np
from jax import lax

D = 2048
HEADS = 16
HEAD_DIM = 128
FF = 1024
TOPK = 8
TOK_DEV = 192
LONGEST = 1024
ATT = 2048
EXPERTS = 32
GROUP = 1536
SEQS = 2
CAP_SRC = 48
SLOTS = 384
N_SEQ = 8
N_FSDP = 4


def with_spikes(values, key, source, target, shards_of, factor):
    def block_of(dim):
        return (jnp.arange(values.shape[dim]) // (values.shape[dim] // shards_of)).reshape((-1,) + (1,) * (values.ndim - 1 - dim))

    near = jax.random.permutation(key, shards_of)[block_of(target)]
    second = (block_of(target) + shards_of // 2) % shards_of
    return jnp.where((block_of(source) == near) | (block_of(source) == second), factor * values, values)


def block_levels(stream_key, dims, split, low, top_value):
    factor_of, own = 1.0, jax.random.fold_in(stream_key, 6)
    for dim, shards_of in split:
        heights = jnp.exp(jax.random.uniform(jax.random.fold_in(own, dim), (shards_of,), jnp.float32, low / len(split), top_value / len(split)))
        factor_of = factor_of * jnp.repeat(heights, dims[dim] // shards_of).reshape([-1 if axis == dim else 1 for axis in range(len(dims))])
    return factor_of


def distinct(own_key, rows, number_of, top, lift):
    ranking = jax.random.permutation(jax.random.fold_in(own_key, 1), number_of)
    favour = ranking
    for power in range(3):
        favour = favour * favour // number_of
    favour = favour * lift // number_of
    chance = jax.random.randint(jax.random.fold_in(own_key, 2), (rows, number_of), 0, 4096) + favour
    holders = jax.random.permutation(jax.random.fold_in(own_key, 3), rows)[jnp.arange(number_of) % rows]
    chance = jnp.where(jnp.arange(rows)[:, None] == holders[None, :], 1 << 14, chance)
    priority = chance * number_of + jnp.arange(number_of)
    return lax.top_k(priority.astype(jnp.int32), top)[1].astype(jnp.int32)


def length_profile(amount, total, bound, skew):
    loads = [(1 << 20) // math.isqrt(standing ** skew) + 1 for standing in range(2, amount + 1)]
    surplus, given = total - bound - (amount - 1), [1] * (amount - 1)
    while surplus > 0:
        movable = [i for i in range(amount - 1) if given[i] < bound]
        pool, remaining = sum([loads[i] for i in movable]), surplus
        for i in movable:
            extra = min(bound - given[i], max(1, remaining * loads[i] // pool), surplus)
            given[i] = given[i] + extra
            surplus = surplus - extra
    return np.array([bound] + given)


def ragged_sizes(rng, count, total, reach, slope):
    if count == 2:
        one = jax.random.randint(rng, (), max(1, total - reach), min(reach, total - 1) + 1)
        return jnp.stack([one, total - one])
    tallies = jnp.asarray(length_profile(count, total, reach, slope), jnp.int32)
    twos = (count - 1) // 2
    donor, sink = tallies[1:1 + 2 * twos:2], tallies[2:2 + 2 * twos:2]
    room = jnp.minimum(donor - 1, reach - sink)
    shifted = jax.random.randint(jax.random.fold_in(rng, 1), (twos,), 0, 1 << 20) % (room + 1)
    tallies = tallies.at[1:1 + 2 * twos:2].set(donor - shifted).at[2:2 + 2 * twos:2].set(sink + shifted)
    return tallies[jax.random.permutation(jax.random.fold_in(rng, 2), count)]


def noise(stream_key, dims, scale, limit, shards=(), kind=jnp.bfloat16):
    drawn = jax.random.normal(stream_key, dims, jnp.float32) * scale
    if len(shards) > 0:
        drawn = block_levels(stream_key, dims, shards, -0.22, 0.18) * drawn
    return jnp.clip(drawn, min=-limit, max=limit).astype(kind)


def heavy_noise(stream_key, shape, spread, bound, pieces, heavy, held_as=jnp.bfloat16):
    values = spread * jax.random.normal(stream_key, shape, jnp.float32)
    if pieces:
        values = values * block_levels(stream_key, shape, pieces, -0.22, 0.18)
    return jnp.clip(with_spikes(values, jax.random.fold_in(stream_key, 3), *heavy), -bound, bound).astype(held_as)


def setup_inputs(seed: int = 0) -> dict:
    key_of = jax.random.split(jax.random.key(seed), 18)
    return {
        "hidden_in": heavy_noise(key_of[0], (N_FSDP, GROUP, D), 1.0, 6.0, ((0, 4), (1, 8)), (1, 2, 8, 2.0)),
        "weight_query": noise(key_of[1], (D, ATT), D ** -0.5, 0.125, ((0, 32),)),
        "weight_key": noise(key_of[2], (D, ATT), D ** -0.5, 0.125, ((0, 32),)),
        "weight_value": noise(key_of[3], (D, ATT), D ** -0.5, 0.125, ((0, 32),)),
        "weight_output": noise(key_of[4], (ATT, D), (max(2, ATT // 256)) ** -0.5, 2.0, ((0, 32),)),
        "weight_router": noise(key_of[5], (D, EXPERTS), (4 * D) ** -0.5, 0.0625, ((0, 32),)),
        "attention_gain": jnp.clip(1.0 + 0.1 * jax.random.normal(key_of[6], (D,), jnp.float32), 0.5, 1.5).astype(jnp.bfloat16),
        "mixture_gain": jnp.clip(1.0 + 0.1 * jax.random.normal(key_of[7], (D,), jnp.float32), 0.5, 1.5).astype(jnp.bfloat16),
        "queries_gain": jnp.clip(1.0 + 0.1 * jax.random.normal(key_of[8], (ATT,), jnp.float32), 0.5, 1.5).astype(jnp.bfloat16),
        "keys_gain": jnp.clip(1.0 + 0.1 * jax.random.normal(key_of[9], (ATT,), jnp.float32), 0.5, 1.5).astype(jnp.bfloat16),
        "weight_gate": noise(key_of[10], (EXPERTS, D, FF), D ** -0.5, 0.125, ((0, 8), (1, 4))),
        "weight_up": noise(key_of[11], (EXPERTS, D, FF), D ** -0.5, 0.125, ((0, 8), (1, 4))),
        "weight_down": noise(key_of[12], (EXPERTS, FF, D), (max(2, FF // 16)) ** -0.5, 0.75, ((0, 8), (1, 4))),
        "cotangent": noise(key_of[13], (N_FSDP, GROUP, D), 1.0, 6.0, ((0, 4), (1, 8))),
        "token_order": jax.vmap(lambda own: jax.random.permutation(own, GROUP))(jax.random.split(key_of[14], N_FSDP)).reshape((N_FSDP, GROUP)).astype(jnp.int32),
        "sequence_lengths": jax.vmap(lambda own: ragged_sizes(own, SEQS, GROUP, LONGEST, 2))(jax.random.split(key_of[15], N_FSDP)).reshape((N_FSDP, SEQS)).astype(jnp.int32),
        "expert_choice": distinct(key_of[16], N_FSDP * GROUP, EXPERTS, TOPK, 4096).reshape((N_FSDP, GROUP, TOPK)),
    }


highest = lax.Precision.HIGHEST
rope_base = 50000.0
norm_eps = 1e-06
masked_score = -1e+30

@jax.custom_vjp
def low(v):
    return lax.optimization_barrier(v.astype(jnp.bfloat16)).astype(jnp.float32)

@jax.custom_vjp
def low_back(v):
    return v

def low_keep(v):
    return (low(v), None)

def low_pass(kept, grad):
    return (grad,)

def back_keep(v):
    return (v, None)

def back_low(kept, grad):
    return (low(grad),)
low.defvjp(low_keep, low_pass)
low_back.defvjp(back_keep, back_low)

def rms_scale(values, scaling):
    return values * lax.rsqrt(lax.optimization_barrier(jnp.mean(values * values, axis=-1, keepdims=True)) + norm_eps) * scaling

def rotate(values, position):
    half_width = values.shape[-1] // 2
    exponents = jnp.arange(half_width, dtype=jnp.float32) * (2.0 / values.shape[-1])
    frequency = jnp.power(rope_base, -exponents)
    angles = position.astype(jnp.float32)[:, None] * frequency[None, :]
    cosine = jnp.cos(angles)[:, None, :]
    sine_table = jnp.sin(angles)[:, None, :]
    first_half = values[..., :half_width]
    second_half = values[..., half_width:]
    return jnp.concatenate([first_half * cosine - second_half * sine_table, second_half * cosine + first_half * sine_table], axis=-1)

def layout(places, lengths):
    cumulative = jnp.cumsum(lengths).astype(jnp.int32)
    starts = (cumulative - lengths).astype(jnp.int32)
    segment = lax.optimization_barrier(jnp.sum((places[:, None] >= cumulative[None, :]).astype(jnp.int32), axis=1)).astype(jnp.int32)
    picked = segment[:, None] == jnp.arange(lengths.shape[0], dtype=jnp.int32)[None, :]
    position = (places - lax.optimization_barrier(jnp.sum(jnp.where(picked, starts[None, :], 0), axis=1))).astype(jnp.int32)
    return (segment, position)

def gate_softmax(logits, chosen_ids):
    picked = chosen_ids[..., None] == jnp.arange(logits.shape[-1], dtype=jnp.int32)
    chosen = lax.optimization_barrier(jnp.sum(jnp.where(picked, logits[:, None, :], 0.0), axis=-1))
    peak_score = lax.optimization_barrier(jnp.max(chosen, axis=-1, keepdims=True))
    weights = jnp.exp(chosen - peak_score)
    return weights / lax.optimization_barrier(jnp.sum(weights, axis=-1, keepdims=True))

def attend(queries, keys, values, segment):
    row_block = min(512, queries.shape[0])
    score_scale = HEAD_DIM ** (-0.5)

    def one_block(block_index):
        query_rows = lax.dynamic_slice_in_dim(queries, block_index * row_block, row_block, 0)
        row_segment = lax.dynamic_slice_in_dim(segment, block_index * row_block, row_block, 0)
        scores = jnp.einsum('qhd,khd->hqk', query_rows, keys, precision=highest) * score_scale
        scores = low_back(jnp.where((row_segment[:, None] == segment[None, :])[None], scores, masked_score))
        peak_score = lax.optimization_barrier(jnp.max(scores, axis=-1, keepdims=True))
        weights = jnp.exp(scores - peak_score)
        probabilities = weights / lax.optimization_barrier(jnp.sum(weights, axis=-1, keepdims=True))
        return jnp.einsum('hqk,khd->qhd', low(probabilities), values, precision=highest)
    outcome = lax.map(jax.checkpoint(one_block), jnp.arange(queries.shape[0] // row_block, dtype=jnp.int32))
    return outcome.reshape(queries.shape)

def group_forward(inputs, dense, experts, places, lengths, chosen_ids):
    weight_query, weight_key, weight_value, weight_output, weight_router, attention_gain, mixture_gain, queries_gain, keys_gain = dense
    weight_gate, weight_up, weight_down = experts
    row_count = inputs.shape[0]
    segment, position = layout(places, lengths)
    normed = low(rms_scale(inputs, attention_gain))
    query_raw = low_back(jnp.dot(normed, weight_query, precision=highest))
    key_raw = low_back(jnp.dot(normed, weight_key, precision=highest))
    value_low = low_back(low(jnp.dot(normed, weight_value, precision=highest)))
    queries = low_back(low(rotate(rms_scale(query_raw, queries_gain).reshape(row_count, HEADS, HEAD_DIM), position)))
    keys = low_back(low(rotate(rms_scale(key_raw, keys_gain).reshape(row_count, HEADS, HEAD_DIM), position)))
    attended = attend(queries, keys, value_low.reshape(row_count, HEADS, HEAD_DIM), segment).reshape(row_count, ATT)
    attended = low_back(low(attended))
    residual = inputs + low_back(jnp.dot(attended, weight_output, precision=highest))
    mixed_low = low(rms_scale(residual, mixture_gain))
    logits = jnp.dot(mixed_low, weight_router, precision=highest)
    gate_weights = gate_softmax(logits, chosen_ids)
    flat_choice = chosen_ids.reshape(N_SEQ, TOK_DEV * TOPK)
    onehot = (flat_choice[..., None] == jnp.arange(EXPERTS, dtype=jnp.int32)).astype(jnp.int32)
    slot_rank = lax.optimization_barrier(jnp.sum((jnp.cumsum(onehot, axis=1) - onehot) * onehot, axis=-1)).astype(jnp.int32)
    slot_kept = slot_rank < CAP_SRC
    source = jnp.arange(N_SEQ, dtype=jnp.int32)[:, None]
    slot_total = EXPERTS * SLOTS
    target = jnp.where(slot_kept, (flat_choice * N_SEQ + source) * CAP_SRC + slot_rank, slot_total)
    target = target.reshape(-1).astype(jnp.int32)
    slot_kept = slot_kept.reshape(-1)
    slot_owner = jnp.zeros((slot_total,), jnp.int32).at[target].set(jnp.arange(GROUP * TOPK, dtype=jnp.int32), mode='drop')
    filled = jnp.zeros((slot_total,), jnp.float32).at[target].set(1.0, mode='drop')
    slot_inputs = low_back(mixed_low[slot_owner // TOPK] * filled[:, None]).reshape(EXPERTS, SLOTS, D)
    gate_act = low_back(jnp.einsum('ecd,edf->ecf', slot_inputs, weight_gate, precision=highest))
    up_act = low_back(jnp.einsum('ecd,edf->ecf', slot_inputs, weight_up, precision=highest))
    hidden_units = low(jax.nn.silu(gate_act) * up_act)
    expert_out = low_back(low(jnp.einsum('ecf,efd->ecd', hidden_units, weight_down, precision=highest)))
    expert_out = expert_out.reshape(slot_total, D)
    safe_slot = jnp.minimum(target, slot_total - 1)
    pair_out = jnp.where(slot_kept[:, None], expert_out[safe_slot], 0.0).reshape(row_count, TOPK, D)
    return residual + lax.optimization_barrier(jnp.sum(gate_weights[..., None] * pair_out, axis=1))

def reference(hidden_in, weight_query, weight_key, weight_value, weight_output, weight_router, attention_gain, mixture_gain, queries_gain, keys_gain, weight_gate, weight_up, weight_down, cotangent, token_order, sequence_lengths, expert_choice):
    dense = tuple((item.astype(jnp.float32) for item in (weight_query, weight_key, weight_value, weight_output, weight_router, attention_gain, mixture_gain, queries_gain, keys_gain)))
    experts = tuple((item.astype(jnp.float32) for item in (weight_gate, weight_up, weight_down)))
    inputs = hidden_in.astype(jnp.float32)

    def forward(inputs, dense, experts):

        def per_group(group_item):
            return group_forward(group_item[0], dense, experts, group_item[1], group_item[2], group_item[3])
        return lax.map(per_group, (inputs, token_order, sequence_lengths, expert_choice))
    result, pull = jax.vjp(forward, inputs, dense, experts)
    grad_inputs, grad_dense, grad_experts = pull(cotangent.astype(jnp.float32))
    return (result.astype(jnp.bfloat16), grad_inputs.astype(jnp.bfloat16), grad_dense[0], grad_dense[1], grad_dense[2], grad_dense[3], grad_dense[4], grad_dense[5], grad_dense[6], grad_dense[7], grad_dense[8], grad_experts[0], grad_experts[1], grad_experts[2])
```

```python
import jax
import jax.numpy as jnp
from jax import lax
from jax.sharding import PartitionSpec as P

HEAD_DIM = 128


highest = lax.Precision.HIGHEST
rope_base = 50000.0
norm_eps = 1e-06
masked_score = -1e30


def rms_scale(values, scaling):
    return (
        values * lax.rsqrt(jnp.mean(values * values, axis=-1, keepdims=True) + norm_eps) * scaling
    )


def rotate(values, position):
    half_width = values.shape[-1] // 2
    exponents = jnp.arange(half_width, dtype=jnp.float32) * (2.0 / values.shape[-1])
    frequency = jnp.power(rope_base, -exponents)
    angles = position.astype(jnp.float32)[:, None] * frequency[None, :]
    cosine = jnp.cos(angles)[:, None, :]
    sine_table = jnp.sin(angles)[:, None, :]
    first_half = values[..., :half_width]
    second_half = values[..., half_width:]
    return jnp.concatenate(
        [
            first_half * cosine - second_half * sine_table,
            second_half * cosine + first_half * sine_table,
        ],
        axis=-1,
    )


def layout(places, lengths):
    cumulative = jnp.cumsum(lengths)
    starts = cumulative - lengths
    segment = jnp.sum((places[:, None] >= cumulative[None, :]).astype(jnp.int32), axis=1)
    picked = segment[:, None] == jnp.arange(lengths.shape[0], dtype=jnp.int32)[None, :]
    position = places - jnp.sum(jnp.where(picked, starts[None, :], 0), axis=1)
    return (segment, position)


def gate_softmax(logits, chosen_ids):
    picked = chosen_ids[..., None] == jnp.arange(logits.shape[-1], dtype=jnp.int32)
    chosen = jnp.sum(jnp.where(picked, logits[:, None, :], 0.0), axis=-1)
    peak_score = jnp.max(chosen, axis=-1, keepdims=True)
    weights = jnp.exp(chosen - peak_score)
    return weights / jnp.sum(weights, axis=-1, keepdims=True)


def norm_rotate(raw_values, scaling, position):
    row_count = raw_values.shape[0]
    normed = rms_scale(raw_values, scaling).reshape(row_count, -1, HEAD_DIM)
    return rotate(normed, position).reshape(row_count, -1)


def score_block(query_rows, row_segment, head_keys, segment, score_scale):
    scores = (
        jnp.einsum("qhd,khd->hqk", query_rows, head_keys, preferred_element_type=jnp.float32)
        * score_scale
    )
    return jnp.where((row_segment[:, None] == segment[None, :])[None], scores, masked_score)


AXES = ("seq", "fsdp")
low_type = jnp.bfloat16


def rotate_back(values, position):
    half_width = values.shape[-1] // 2
    exponents = jnp.arange(half_width, dtype=jnp.float32) * (2.0 / values.shape[-1])
    frequency = jnp.power(rope_base, -exponents)
    angles = position.astype(jnp.float32)[:, None] * frequency[None, :]
    cosine = jnp.cos(angles)[:, None, :]
    sine_table = jnp.sin(angles)[:, None, :]
    first_half = values[..., :half_width]
    second_half = values[..., half_width:]
    return jnp.concatenate(
        [
            first_half * cosine + second_half * sine_table,
            second_half * cosine - first_half * sine_table,
        ],
        axis=-1,
    )


def swap(values, axis_name, dim):
    return lax.all_to_all(values, axis_name, split_axis=dim, concat_axis=dim, tiled=True)


def dot32(spec, left, right):
    return jnp.einsum(spec, left, right, preferred_element_type=jnp.float32)


def attention_forward(head_queries, head_keys, head_values, segment, score_scale):
    group = head_queries.shape[0]
    row_block = min(512, group)
    block_count = group // row_block

    def forward_block(block_index):
        row_start = block_index * row_block
        query_rows = lax.dynamic_slice_in_dim(head_queries, row_start, row_block, 0)
        row_segment = lax.dynamic_slice_in_dim(segment, row_start, row_block, 0)
        scores = score_block(query_rows, row_segment, head_keys, segment, score_scale)
        peak_score = jnp.max(scores, axis=-1, keepdims=True)
        weights = jnp.exp(scores - peak_score)
        totals = jnp.sum(weights, axis=-1, keepdims=True)
        probabilities = (weights / totals).astype(low_type)
        outcome = dot32("hqk,khd->qhd", probabilities, head_values)
        return (outcome.astype(low_type), (peak_score + jnp.log(totals))[..., 0])

    outcome, log_totals = lax.map(forward_block, jnp.arange(block_count, dtype=jnp.int32))
    return outcome.reshape(group, -1), log_totals


def attention_backward(head_queries, head_keys, head_values, grad_heads, segment, log_totals, score_scale):
    group = head_queries.shape[0]
    row_block = min(512, group)
    block_count = group // row_block

    def backward_block(running, block_inputs):
        grad_key_sum, grad_value_sum = running
        block_index, log_total = block_inputs
        row_start = block_index * row_block
        query_rows = lax.dynamic_slice_in_dim(head_queries, row_start, row_block, 0)
        row_segment = lax.dynamic_slice_in_dim(segment, row_start, row_block, 0)
        grad_rows = lax.dynamic_slice_in_dim(grad_heads, row_start, row_block, 0)
        scores = score_block(query_rows, row_segment, head_keys, segment, score_scale)
        probabilities = jnp.exp(scores - log_total[..., None])
        grad_probs = dot32("qhd,khd->hqk", grad_rows, head_values)
        inner_sum = jnp.sum(probabilities * grad_probs, axis=-1, keepdims=True)
        grad_scores = (probabilities * (grad_probs - inner_sum)).astype(low_type)
        grad_query_rows = dot32("hqk,khd->qhd", grad_scores, head_keys) * score_scale
        grad_key_sum = grad_key_sum + dot32("hqk,qhd->khd", grad_scores, query_rows) * score_scale
        grad_value_sum = grad_value_sum + dot32(
            "hqk,qhd->khd", probabilities.astype(low_type), grad_rows
        )
        return ((grad_key_sum, grad_value_sum), grad_query_rows)

    zero_heads = jnp.zeros(head_keys.shape, jnp.float32)
    (grad_keys, grad_values), grad_queries = lax.scan(
        backward_block,
        (zero_heads, zero_heads),
        (jnp.arange(block_count, dtype=jnp.int32), log_totals),
    )
    return grad_queries.reshape(head_queries.shape), grad_keys, grad_values


def body(
    hidden_in,
    weight_query,
    weight_key,
    weight_value,
    weight_output,
    weight_router,
    attention_gain,
    mixture_gain,
    queries_gain,
    keys_gain,
    weight_gate,
    weight_up,
    weight_down,
    cotangent,
    token_order,
    sequence_lengths,
    expert_choice,
):
    seq_count = lax.axis_size("seq")
    seq_place = lax.axis_index("seq")
    fsdp_count = lax.axis_size("fsdp")
    fsdp_place = lax.axis_index("fsdp")
    inputs_low = hidden_in[0]
    tokens, width = inputs_low.shape
    group = tokens * seq_count
    shard_rows, columns_all = weight_query.shape
    columns = columns_all // seq_count
    local_heads = columns // HEAD_DIM
    score_scale = HEAD_DIM ** (-0.5)
    chosen_ids = expert_choice[0]
    top_count = chosen_ids.shape[1]

    small = jnp.concatenate(
        [
            weight_router,
            attention_gain[:, None],
            mixture_gain[:, None],
            queries_gain[:, None],
            keys_gain[:, None],
        ],
        axis=1,
    )
    small = lax.all_gather(small, AXES, axis=0, tiled=True)
    experts_all = weight_router.shape[1]
    full_router = small[:, :experts_all]
    norm_first = small[:, experts_all].astype(jnp.float32)
    norm_second = small[:, experts_all + 1].astype(jnp.float32)
    own_columns = lax.dynamic_slice_in_dim(
        small[:, experts_all + 2 :].astype(jnp.float32), seq_place * columns, columns, 0
    )
    norm_queries, norm_keys = own_columns[:, 0], own_columns[:, 1]

    inputs_group = lax.all_gather(inputs_low, "seq", axis=0, tiled=True).astype(jnp.float32)
    qkv_parts = jnp.stack(
        [w.reshape(shard_rows, seq_count, columns) for w in (weight_query, weight_key, weight_value)]
    )
    qkv_parts = swap(qkv_parts.transpose(2, 0, 1, 3), "seq", 0)
    qkv_parts = lax.all_gather(qkv_parts, "fsdp", axis=0, tiled=False)
    weight_qkv = qkv_parts.transpose(1, 0, 3, 2, 4).reshape(width, 3 * columns)
    full_output = lax.all_gather(weight_output, AXES, axis=0, tiled=True)

    local_experts, row_share, hidden_count = weight_gate.shape
    parts = fsdp_count // local_experts
    assert parts * local_experts == fsdp_count
    strip = hidden_count // (fsdp_count * parts)

    def to_owner(weights):
        pieces = weights.reshape(local_experts, row_share, fsdp_count, parts, strip)
        pieces = pieces.transpose(0, 3, 1, 2, 4)
        pieces = pieces.reshape(fsdp_count, row_share, fsdp_count * strip)
        return swap(pieces, "fsdp", 0).reshape(width, fsdp_count * strip)

    def from_owner(grads):
        pieces = grads.reshape(fsdp_count, row_share, fsdp_count * strip)
        pieces = swap(pieces, "fsdp", 0)
        pieces = pieces.reshape(local_experts, parts, row_share, fsdp_count, strip)
        pieces = pieces.transpose(0, 2, 3, 1, 4)
        return pieces.reshape(local_experts, row_share, hidden_count).astype(jnp.float32)

    own_down = swap(weight_down.reshape(fsdp_count, strip, width), "fsdp", 0).reshape(-1, width)
    own_gate = to_owner(weight_gate)
    own_up = to_owner(weight_up)

    capacity = tokens * top_count // experts_all
    lanes = seq_count * capacity
    lane = jnp.arange(lanes, dtype=jnp.int32)
    lane_expert = lane // capacity * local_experts + fsdp_place // parts
    lane_slot = (lane % capacity).astype(jnp.float32)
    choice_all = lax.all_gather(chosen_ids, "fsdp", axis=0, tiled=False)
    named = jnp.any(choice_all[..., None] == lane_expert, axis=2)
    earlier = (
        jnp.arange(tokens, dtype=jnp.int32)[:, None] > jnp.arange(tokens, dtype=jnp.int32)[None, :]
    ).astype(low_type)
    rank = dot32("tu,guj->gtj", earlier, named.astype(low_type))
    holds = named & (rank == lane_slot)
    place = holds.astype(low_type)

    def to_slots(rows):
        sent = jnp.einsum("gtj,gtd->gjd", place, rows)
        sent = sent.reshape(fsdp_count, seq_count, capacity, width)
        return swap(sent, "seq", 1).reshape(fsdp_count * lanes, width)

    def from_slots(rows, matrix):
        back = swap(rows.reshape(fsdp_count, seq_count, capacity, width), "seq", 1)
        mixed = dot32("gtj,gjd->gtd", matrix, back.reshape(fsdp_count, lanes, width))
        parts_back = swap(mixed.astype(low_type), "fsdp", 0)
        return jnp.sum(parts_back.astype(jnp.float32), axis=0)

    cotangent_low = cotangent[0]
    cotangent_all = lax.all_gather(cotangent_low, "fsdp", axis=0, tiled=False)
    slot_cotangent = to_slots(cotangent_all)
    units_cotangent = dot32("cd,fd->cf", slot_cotangent, own_down)

    segment, position = layout(token_order[0], sequence_lengths[0])
    first_scale = lax.rsqrt(jnp.mean(inputs_group * inputs_group, axis=-1, keepdims=True) + norm_eps)
    normed = (inputs_group * first_scale * norm_first).astype(low_type)
    raw = dot32("td,dc->tc", normed, weight_qkv)
    query_raw, key_raw = raw[:, :columns], raw[:, columns : 2 * columns]
    head_values = raw[:, 2 * columns :].astype(low_type).reshape(group, local_heads, HEAD_DIM)

    def group_means(left, right):
        sums = jnp.stack([jnp.sum(left, axis=-1), jnp.sum(right, axis=-1)])
        sums = jnp.sum(lax.all_gather(sums, "seq", axis=0, tiled=False), axis=0)
        return (sums / columns_all)[..., None]

    squares = group_means(query_raw * query_raw, key_raw * key_raw)
    query_scale, key_scale = lax.rsqrt(squares[0] + norm_eps), lax.rsqrt(squares[1] + norm_eps)
    query_unit, key_unit = query_raw * query_scale, key_raw * key_scale

    def spin(values, scaling):
        return rotate((values * scaling).reshape(group, -1, HEAD_DIM), position).astype(low_type)

    head_queries, head_keys = spin(query_unit, norm_queries), spin(key_unit, norm_keys)
    attended_heads, log_totals = attention_forward(
        head_queries, head_keys, head_values, segment, score_scale
    )
    attended = lax.all_to_all(attended_heads, "seq", split_axis=0, concat_axis=1, tiled=True)
    inputs = inputs_low.astype(jnp.float32)
    residual = inputs + dot32("ta,ad->td", attended, full_output)

    second_scale = lax.rsqrt(jnp.mean(residual * residual, axis=-1, keepdims=True) + norm_eps)
    second_unit = residual * second_scale
    mixed_low = (second_unit * norm_second).astype(low_type)
    mixed_all = lax.all_gather(mixed_low, "fsdp", axis=0, tiled=False)
    logits = dot32("td,de->te", mixed_low, full_router)
    gate_weights = gate_softmax(logits, chosen_ids)
    gates_all = lax.all_gather(gate_weights, "fsdp", axis=0, tiled=False)
    lane_gate = jnp.sum(
        jnp.where(choice_all[..., None] == lane_expert, gates_all[..., None], 0.0), axis=2
    )
    place_gate = jnp.where(holds, lane_gate, 0.0)
    slot_gate = jnp.sum(place_gate, axis=1).reshape(fsdp_count, seq_count, capacity)
    slot_gate = swap(slot_gate, "seq", 1).reshape(-1, 1)

    slot_inputs = to_slots(mixed_all)
    gate_act = dot32("cd,df->cf", slot_inputs, own_gate)
    up_act = dot32("cd,df->cf", slot_inputs, own_up)
    sigma = jax.nn.sigmoid(gate_act)
    silu = gate_act * sigma
    hidden_units = (silu * up_act).astype(low_type)

    grad_units = slot_gate * units_cotangent
    grad_gate_low = (grad_units * up_act * sigma * (1.0 + gate_act * (1.0 - sigma))).astype(low_type)
    grad_up_low = (grad_units * silu).astype(low_type)
    grad_slots_in = dot32("cf,df->cd", grad_gate_low, own_gate)
    grad_slots_in = (grad_slots_in + dot32("cf,df->cd", grad_up_low, own_up)).astype(low_type)
    from_pairs = from_slots(grad_slots_in, place)

    slot_grad_gate = jnp.sum(hidden_units.astype(jnp.float32) * units_cotangent, axis=-1)
    slot_grad_gate = swap(slot_grad_gate.reshape(fsdp_count, seq_count, capacity), "seq", 1)
    lane_grad = jnp.where(holds, slot_grad_gate.reshape(fsdp_count, 1, lanes), 0.0)
    grad_gates = jnp.sum(
        jnp.where(choice_all[..., None] == lane_expert, lane_grad[:, :, None, :], 0.0), axis=-1
    )
    grad_gates = jnp.sum(swap(grad_gates, "fsdp", 0), axis=0)
    pair_logits = gate_weights * (
        grad_gates - jnp.sum(gate_weights * grad_gates, axis=-1, keepdims=True)
    )
    picked = chosen_ids[..., None] == jnp.arange(experts_all, dtype=jnp.int32)
    grad_logits = jnp.sum(jnp.where(picked, pair_logits[..., None], 0.0), axis=1)

    grad_mixed = from_pairs + jnp.dot(
        grad_logits, full_router.astype(jnp.float32).T, precision=highest
    )
    grad_router = jnp.dot(mixed_low.astype(jnp.float32).T, grad_logits, precision=highest)
    upstream = cotangent_low.astype(jnp.float32)
    scaled = norm_second * grad_mixed
    grad_residual = upstream + second_scale * (
        scaled - second_unit * jnp.mean(second_unit * scaled, axis=-1, keepdims=True)
    )
    grad_mixture_gain = jnp.sum(grad_mixed * second_unit, axis=0)
    grad_branch = grad_residual.astype(low_type)

    grad_attended = dot32("td,ad->ta", grad_branch, full_output).astype(low_type)
    grad_heads = lax.all_to_all(
        grad_attended, "seq", split_axis=1, concat_axis=0, tiled=True
    ).reshape(group, local_heads, HEAD_DIM)
    grad_branch_group = lax.all_gather(grad_branch, "seq", axis=0, tiled=True)

    grad_gate = from_owner(dot32("cd,cf->df", slot_inputs, grad_gate_low).astype(low_type))
    grad_up = from_owner(dot32("cd,cf->df", slot_inputs, grad_up_low).astype(low_type))
    gated_units = (slot_gate * hidden_units.astype(jnp.float32)).astype(low_type)
    down_term = dot32("cf,cd->fd", gated_units, slot_cotangent).astype(low_type)
    grad_down = swap(down_term.reshape(fsdp_count, strip, width), "fsdp", 0)
    grad_down = grad_down.reshape(local_experts, parts * strip, width).astype(jnp.float32)

    expert_out = dot32("cf,fd->cd", hidden_units, own_down).astype(low_type)
    block_out = residual + from_slots(expert_out, place_gate.astype(low_type))

    grad_queries, grad_keys, grad_values = attention_backward(
        head_queries, head_keys, head_values, grad_heads, segment, log_totals, score_scale
    )

    query_back = rotate_back(grad_queries, position).reshape(group, columns)
    key_back = rotate_back(grad_keys, position).reshape(group, columns)
    grad_norms = jnp.concatenate(
        [jnp.sum(query_back * query_unit, axis=0), jnp.sum(key_back * key_unit, axis=0)]
    ).reshape(2, columns)
    query_back, key_back = query_back * norm_queries, key_back * norm_keys
    inner = group_means(query_back * query_unit, key_back * key_unit)
    grad_raw = jnp.concatenate(
        [
            (query_scale * (query_back - query_unit * inner[0])).astype(low_type),
            (key_scale * (key_back - key_unit * inner[1])).astype(low_type),
            grad_values.reshape(group, columns).astype(low_type),
        ],
        axis=1,
    )
    normed_part = dot32("tc,dc->td", grad_raw, weight_qkv).astype(low_type)
    normed_parts = swap(normed_part.reshape(seq_count, tokens, width), "seq", 0)
    grad_normed = jnp.sum(normed_parts.astype(jnp.float32), axis=0)
    own_scale = lax.rsqrt(jnp.mean(inputs * inputs, axis=-1, keepdims=True) + norm_eps)
    first_unit = inputs * own_scale
    grad_attention_gain = jnp.sum(grad_normed * first_unit, axis=0)
    scaled = norm_first * grad_normed
    grad_hidden = (
        grad_residual
        + own_scale * (scaled - first_unit * jnp.mean(first_unit * scaled, axis=-1, keepdims=True))
    ).astype(low_type)

    grad_output = dot32("ta,td->ad", attended_heads, grad_branch_group).astype(low_type)
    grad_output = swap(grad_output.reshape(fsdp_count, shard_rows, width), "fsdp", 0)
    grad_output = jnp.sum(grad_output.astype(jnp.float32), axis=0)
    grad_qkv = dot32("td,tc->dc", normed, grad_raw).astype(low_type)
    grad_qkv = grad_qkv.reshape(seq_count, fsdp_count, shard_rows, 3 * columns)
    grad_qkv = jnp.sum(swap(grad_qkv, "fsdp", 1).astype(jnp.float32), axis=1).astype(low_type)
    grad_qkv = swap(grad_qkv, "seq", 0).reshape(seq_count, shard_rows, 3, columns)
    grad_qkv = grad_qkv.transpose(2, 1, 0, 3).reshape(3, shard_rows, columns_all)
    grad_qkv = grad_qkv.astype(jnp.float32)

    grad_norms = lax.psum_scatter(grad_norms, "fsdp", scatter_dimension=1, tiled=True)
    rows_sum = jnp.concatenate(
        [grad_router, grad_attention_gain[:, None], grad_mixture_gain[:, None]], axis=1
    )
    rows_sum = lax.psum_scatter(rows_sum, AXES, scatter_dimension=0, tiled=True)
    return (
        block_out.astype(low_type)[None],
        grad_hidden[None],
        grad_qkv[0],
        grad_qkv[1],
        grad_qkv[2],
        grad_output,
        rows_sum[:, :experts_all],
        rows_sum[:, experts_all],
        rows_sum[:, experts_all + 1],
        grad_norms[0],
        grad_norms[1],
        grad_gate,
        grad_up,
        grad_down,
    )


def solution(mesh):
    placed = (
        P("fsdp", "seq", None),
        P(("seq", "fsdp"), None),
        P(("seq", "fsdp"), None),
        P(("seq", "fsdp"), None),
        P(("seq", "fsdp"), None),
        P(("seq", "fsdp"), None),
        P(("seq", "fsdp")),
        P(("seq", "fsdp")),
        P(("seq", "fsdp")),
        P(("seq", "fsdp")),
        P("seq", "fsdp", None),
        P("seq", "fsdp", None),
        P("seq", "fsdp", None),
        P("fsdp", "seq", None),
        P("fsdp", None),
        P("fsdp", None),
        P("fsdp", "seq", None),
    )
    return jax.shard_map(
        body,
        mesh=mesh,
        in_specs=placed,
        out_specs=(
            P("fsdp", "seq", None),
            P("fsdp", "seq", None),
            P(("seq", "fsdp"), None),
            P(("seq", "fsdp"), None),
            P(("seq", "fsdp"), None),
            P(("seq", "fsdp"), None),
            P(("seq", "fsdp"), None),
            P(("seq", "fsdp")),
            P(("seq", "fsdp")),
            P(("seq", "fsdp")),
            P(("seq", "fsdp")),
            P("seq", "fsdp", None),
            P("seq", "fsdp", None),
            P("seq", "fsdp", None),
        ),
        check_vma=False,
    )
```
